32 devices in a mesh: sector: 16 (over z, y, x), block: 2 (over core).
Axes of the slice: x: 2, y: 2, z: 4, core: 2. Of those that a mesh axis runs over, the one named last changes fastest.
Arguments:
- adjoint_prev: float32 [5, 16, 128, 128], P(None, 'block', 'sector'), may hold values from -6 to 6
- adjoint_source: float32 [5, 16, 128, 128], P(None, 'block', 'sector'), may hold values from -6 to 6
- face_matrices: bfloat16 [3, 5, 5, 16, 128, 128], P(None, None, None, 'block', 'sector'), may hold values from -2.5 to 2.5
- inverse_blocks: bfloat16 [5, 5, 16, 128, 128], P(None, None, 'block', 'sector')
- sector_offset: int32 [1], replicated, may hold values from 1 to 15
- donor_cells: int32 [128], P('sector'), may hold values from 0 to 7
- donor_weights: float32 [128], P('sector'), may hold values from 0.1 to 0.9
Outputs:
- adjoint: float32 [5, 16, 128, 128], P(None, 'block', 'sector')
- last_update: float32 [5, 16, 128, 128], P(None, 'block', 'sector')
The draws below stay inside these ranges and needn't reach their ends.
All inputs are finite; a program needn't handle non-finite values.
Results may differ from the reference program's by a relative error of at most 0.0003.
Values sent between devices are 32-bit elements; how exact they have to be, the bound alone decides.
No kernel may reach another device: no remote copies, remote signals or barrier semaphores. Data moves between devices by JAX's collectives and lax.ppermute only.
A program may use at most 64 MiB of HBM per device.

```python
import jax
import jax.numpy as jnp

CT = 8
NRAD = 128
ITERS = 4
NAX = 16
NCIRC = 128
N_SECTOR = 16


def draw_inverse_blocks(key, part):
    key_off = jax.random.fold_in(key, 11)
    key_diag = jax.random.fold_in(key, 12)
    off_part = 0.06 * jax.random.normal(key_off, (5, 5, NAX, NCIRC, NRAD), jnp.float32)
    diag_part = jnp.exp(jax.random.uniform(key_diag, (5, NAX, NCIRC, NRAD), jnp.float32, jnp.log(0.15), jnp.log(0.3)))
    identity = jnp.eye(5, dtype=jnp.float32)[:, :, None, None, None]
    return (off_part * (1.0 - identity) + identity * diag_part[:, None]).astype(jnp.bfloat16)


def touch_ends(values, key, least, largest):
    longest = values.shape.index(max(values.shape))
    spots = []
    for shift in (0, 1):
        where = [jax.random.randint(jax.random.fold_in(key, axis), (), 0, length) for axis, length in enumerate(values.shape)]
        where[longest] = (where[longest] + shift) % values.shape[longest]
        spots.append(tuple(where))
    return values.at[spots[0]].set(least).at[spots[1]].set(largest)


def block_scale(rng, shape, pieces, low, largest):
    loudness = 1.0
    for dim, blocks in pieces:
        steps = jax.random.uniform(jax.random.fold_in(jax.random.fold_in(rng, 6), dim), (blocks,), jnp.float32, low / len(pieces), largest / len(pieces))
        loudness = loudness * jnp.repeat(jnp.exp(steps), shape[dim] // blocks).reshape((-1,) + (1,) * (len(shape) - 1 - dim))
    return loudness


def scatter_about(key, extent, deviation, reach, shards=(), kind=jnp.bfloat16):
    factor_of = block_scale(key, extent, shards, -0.22, 0.18) if shards else 1.0
    array = jax.random.normal(key, extent, jnp.float32) * deviation * factor_of
    return jnp.minimum(jnp.maximum(array, -reach), reach).astype(kind)


def setup_inputs(seed: int = 0) -> dict:
    streams_of = jax.random.split(jax.random.key(seed), 8)
    return {
        "adjoint_prev": scatter_about(streams_of[0], (5, NAX, NCIRC, NRAD), 1.0, 6.0, ((1, 2), (2, 16)), jnp.float32),
        "adjoint_source": scatter_about(streams_of[1], (5, NAX, NCIRC, NRAD), 1.0, 6.0, ((1, 2), (2, 16)), jnp.float32),
        "face_matrices": scatter_about(streams_of[2], (3, 5, 5, NAX, NCIRC, NRAD), 5 ** -0.5, 2.5, ((3, 2), (4, 16))),
        "inverse_blocks": draw_inverse_blocks(jax.random.fold_in(streams_of[7], 71), 0),
        "sector_offset": jax.random.randint(streams_of[4], (1,), 1, N_SECTOR).astype(jnp.int32),
        "donor_cells": touch_ends(jax.random.randint(streams_of[5], (NCIRC,), 0, CT), jax.random.fold_in(streams_of[5], 1), 0, CT - 1).astype(jnp.int32),
        "donor_weights": jnp.clip(0.1 + 0.79999997 * jax.random.uniform(streams_of[6], (NCIRC,), jnp.float32) ** block_scale(streams_of[6], (NCIRC,), ((0, 16),), -0.2, 0.2), 0.1, 0.9),
    }


def neighbour_terms(adjoint, sector_offset, donor_cells, donor_weights):
    first = NAX // 2
    rotor_row = adjoint[:, first - 1]
    shift_cells = sector_offset[0] * CT
    base = (jnp.arange(NCIRC, dtype=jnp.int32) // CT) * CT + donor_cells
    source_one = jnp.mod(base - shift_cells, NCIRC).astype(jnp.int32)
    source_two = jnp.mod(base + 1 - shift_cells, NCIRC).astype(jnp.int32)
    weights = donor_weights[None, :, None]
    facing = weights * jnp.take(rotor_row, source_one, axis=1) + (1.0 - weights) * jnp.take(rotor_row, source_two, axis=1)
    zero_layer = jnp.zeros_like(adjoint[:, :1])
    axial_minus = jnp.concatenate([zero_layer, adjoint[:, :-1]], axis=1)
    axial_minus = axial_minus.at[:, first].set(facing)
    axial_plus = jnp.concatenate([adjoint[:, 1:], zero_layer], axis=1)
    around_minus = jnp.roll(adjoint, 1, axis=2)
    around_plus = jnp.roll(adjoint, -1, axis=2)
    padded = jnp.pad(adjoint, ((0, 0), (0, 0), (0, 0), (1, 1)))
    radial_minus = padded[:, :, :, :-2]
    radial_plus = padded[:, :, :, 2:]
    return (0.6 * axial_minus + 0.4 * axial_plus,
            0.6 * around_minus + 0.4 * around_plus,
            0.6 * radial_minus + 0.4 * radial_plus)


def sweep(adjoint, adjoint_source, face_matrices, inverse_blocks, sector_offset, donor_cells, donor_weights):
    mixed = neighbour_terms(adjoint, sector_offset, donor_cells, donor_weights)
    coupled = jnp.zeros_like(adjoint)
    for direction in range(3):
        for comp in range(5):
            coupled = coupled + face_matrices[direction, comp].astype(jnp.float32) * mixed[direction][comp][None]
    total = adjoint_source + coupled
    result = jnp.zeros_like(adjoint)
    for comp in range(5):
        result = result + inverse_blocks[:, comp].astype(jnp.float32) * total[comp][None]
    return result


def reference(adjoint_prev, adjoint_source, face_matrices, inverse_blocks, sector_offset, donor_cells, donor_weights):
    adjoint = adjoint_prev
    last_update = jnp.zeros_like(adjoint_prev)
    for sweep_number in range(ITERS):
        result = sweep(adjoint, adjoint_source, face_matrices, inverse_blocks, sector_offset, donor_cells, donor_weights)
        last_update = result - adjoint
        adjoint = result
    return adjoint, last_update
```

```python
import jax
import jax.numpy as jnp
from jax import lax
from jax.sharding import PartitionSpec as P

ITERS = 4
AXES = ("sector", "block")


def solution(mesh):
    sectors, blocks = mesh.shape["sector"], mesh.shape["block"]
    half = blocks // 2

    def at(s, b):
        return (s % sectors) * blocks + b

    def around(step):
        return [(at(s, b), at(s + step, b)) for s in range(sectors) for b in range(blocks)]

    from_above = [(at(s, b), at(s, b - 1)) for s in range(sectors) for b in range(1, blocks)]

    def from_below(offset):
        return [
            (at(s, b), at(s + (offset if b + 1 == half else 0), b + 1))
            for s in range(sectors)
            for b in range(blocks - 1)
        ]

    def axial_exchange(first, last, offset, block_index):
        if blocks == 2:
            sent = jnp.where(block_index == 0, last, first)
            got = lax.ppermute(sent, AXES, from_above + from_below(offset))
            zero = jnp.zeros_like(got)
            return got, jnp.where(block_index == 0, zero, got), jnp.where(block_index == 0, got, zero)
        below = lax.ppermute(last, AXES, from_below(offset))
        return below, below, lax.ppermute(first, AXES, from_above)

    def sweeps(offset, adjoint, source, face, inverse, table):
        block_index = lax.axis_index("block")
        layers, cells = adjoint.shape[1], adjoint.shape[2]

        def sweep(_, carry):
            adjoint, _ = carry
            row, below, above = axial_exchange(adjoint[:, 0], adjoint[:, -1], offset, block_index)
            minus = lax.ppermute(adjoint[:, :, -1], AXES, around(1))
            head = jnp.concatenate([adjoint[:, :, 0], row[:, :1]], axis=1)
            plus = lax.ppermute(head, AXES, around(-1))
            facing_row = jnp.concatenate([row, plus[:, layers:]], axis=1)
            facing = jnp.einsum("jk,nkr->njr", table, facing_row, precision=lax.Precision.HIGHEST)
            below = jnp.where(block_index == half, facing, below)
            axial_minus = jnp.concatenate([below[:, None], adjoint[:, :-1]], axis=1)
            axial_plus = jnp.concatenate([adjoint[:, 1:], above[:, None]], axis=1)
            around_minus = jnp.concatenate([minus[:, :, None], adjoint[:, :, :-1]], axis=2)
            around_plus = jnp.concatenate([adjoint[:, :, 1:], plus[:, :layers, None]], axis=2)
            radial = jnp.pad(adjoint, ((0, 0), (0, 0), (0, 0), (1, 1)))
            mixed = (
                0.6 * axial_minus + 0.4 * axial_plus,
                0.6 * around_minus + 0.4 * around_plus,
                0.6 * radial[:, :, :, :-2] + 0.4 * radial[:, :, :, 2:],
            )
            total = source
            for direction in range(3):
                for comp in range(5):
                    total = total + face[direction, comp].astype(jnp.float32) * mixed[direction][comp][None]
            result = jnp.zeros_like(adjoint)
            for comp in range(5):
                result = result + inverse[:, comp].astype(jnp.float32) * total[comp][None]
            return result, adjoint

        adjoint, previous = lax.fori_loop(0, ITERS, sweep, (adjoint, adjoint))
        return adjoint, adjoint - previous

    def shards(adjoint_prev, adjoint_source, face, inverse, sector_offset, donor_cells, donor_weights):
        columns = jnp.arange(adjoint_prev.shape[2] + 1, dtype=jnp.int32)
        first_hit = (columns[None, :] == donor_cells[:, None]).astype(jnp.float32)
        second_hit = (columns[None, :] == donor_cells[:, None] + 1).astype(jnp.float32)
        table = donor_weights[:, None] * first_hit + (1.0 - donor_weights[:, None]) * second_hit
        branches = [
            lambda *args, offset=offset: sweeps(offset, *args) for offset in range(1, sectors)
        ]
        return lax.switch(
            sector_offset[0] - 1, branches, adjoint_prev, adjoint_source, face, inverse, table
        )

    return jax.shard_map(
        shards,
        mesh=mesh,
        in_specs=(
            P(None, "block", "sector", None),
            P(None, "block", "sector", None),
            P(None, None, None, "block", "sector", None),
            P(None, None, "block", "sector", None),
            P(),
            P("sector"),
            P("sector"),
        ),
        out_specs=(P(None, "block", "sector", None), P(None, "block", "sector", None)),
        check_vma=False,
    )
```
